32 devices in a mesh: shard: 4 (over z), width: 2 (over core), unit: 4 (over y, x).
Axes of the slice: x: 2, y: 2, z: 4, core: 2. Of those that a mesh axis runs over, the one named last changes fastest.
Arguments:
- w_gate: bfloat16 [14336, 14336], P(('unit', 'shard'), 'width'), parts along dimension 0, may hold values from -0.125 to 0.125
- low_gate: bfloat16 [14336, 64], P(('unit', 'shard')), parts along dimension 0, may hold values from -0.09375 to 0.09375
- high_gate: bfloat16 [256, 14336], P('unit', 'width'), parts along dimension 0, may hold values from -0.75 to 0.75
- w_up: bfloat16 [14336, 14336], P(('unit', 'shard'), 'width'), parts along dimension 0, may hold values from -0.125 to 0.125
- low_up: bfloat16 [14336, 64], P(('unit', 'shard')), parts along dimension 0, may hold values from -0.09375 to 0.09375
- high_up: bfloat16 [256, 14336], P('unit', 'width'), parts along dimension 0, may hold values from -0.75 to 0.75
- norm_train: float32 [14336], P(('unit', 'shard', 'width')), parts along dimension 0, may hold values from 0.25 to 1.75
- norm_step: float32 [14336], P(('unit', 'shard', 'width')), parts along dimension 0, may hold values from -0.3 to 0.3
Outputs:
- serve_gate: bfloat16 [14336, 14336], P('unit', ('width', 'shard')), parts along dimension 0
- serve_up: bfloat16 [14336, 14336], P('unit', ('width', 'shard')), parts along dimension 0
- column_gate: float32 [57344], P(('unit', 'width', 'shard')), parts along dimension 0
- column_up: float32 [57344], P(('unit', 'width', 'shard')), parts along dimension 0
- serve_norm: bfloat16 [14336], P('unit'), parts along dimension 0
The draws below stay inside these ranges and needn't reach their ends.
There are 4 independent parts, one for each index of `unit`. The reference program is written for one: setup_inputs(seed, part) draws one part's arguments, and reference() takes and returns one part's arrays. A program takes and returns all parts, laid end to end along the dimension named above; each array names one. Nothing has to cross between parts.
All inputs are finite; a program needn't handle non-finite values. Where the reference program divides by a largest or mean magnitude, that divisor is 1e-20 or more.
Results may differ from the reference program's by a relative error of at most 0.001.
Values may be sent and summed in bfloat16 or wider, within the bound.
A program may use at most 192 MiB of HBM per device.

```python
import jax
import jax.numpy as jnp

D_MODEL = 3584
D_INNER = 14336
RANK = 64


def spiked(array, stream_key, source, target, blocks, factor):
    def block_of(dim):
        return (jnp.arange(array.shape[dim]) // (array.shape[dim] // blocks)).reshape((-1,) + (1,) * (array.ndim - 1 - dim))

    first = jax.random.permutation(stream_key, blocks)[block_of(target)]
    other_side = (block_of(target) + blocks // 2) % blocks
    return jnp.where((block_of(source) == first) | (block_of(source) == other_side), factor * array, array)


def levels(key, shape, split, low, largest):
    level, own = 1.0, jax.random.fold_in(key, 6)
    for axis_at, blocks in split:
        draws = jnp.exp(jax.random.uniform(jax.random.fold_in(own, axis_at), (blocks,), jnp.float32, low / len(split), largest / len(split)))
        level = level * jnp.repeat(draws, shape[axis_at] // blocks).reshape([-1 if axis == axis_at else 1 for axis in range(len(shape))])
    return level


def bell_draw(rng, dims, width, limit, pieces=(), kind=jnp.bfloat16):
    entries = width * jax.random.normal(rng, dims, jnp.float32)
    if pieces:
        entries = entries * levels(rng, dims, pieces, -0.22, 0.18)
    return jnp.clip(entries, -limit, limit).astype(kind)


def noise_with(own_key, extent, scale, bound, split, heavy, held_as=jnp.bfloat16):
    values = scale * jax.random.normal(own_key, extent, jnp.float32)
    if split:
        values = values * levels(own_key, extent, split, -0.22, 0.18)
    return jnp.clip(spiked(values, jax.random.fold_in(own_key, 3), *heavy), -bound, bound).astype(held_as)


def setup_inputs(seed: int = 0, part: int = 0) -> dict:
    keys = jax.random.split(jax.random.key(seed), 9)
    own_keys = jax.random.split(jax.random.fold_in(keys[8], part), 9)
    return {
        "w_gate": noise_with(own_keys[0], (D_MODEL, D_INNER), D_MODEL ** -0.5, 0.125, ((0, 4), (1, 2)), (0, 1, 4, 2.0)),
        "low_gate": bell_draw(own_keys[1], (D_MODEL, RANK), D_MODEL ** -0.5, 0.09375, ((0, 4),)),
        "high_gate": bell_draw(own_keys[2], (RANK, D_INNER), RANK ** -0.5, 0.75, ((1, 2),)),
        "w_up": noise_with(own_keys[3], (D_MODEL, D_INNER), D_MODEL ** -0.5, 0.125, ((0, 4), (1, 2)), (0, 1, 4, 2.0)),
        "low_up": bell_draw(own_keys[4], (D_MODEL, RANK), D_MODEL ** -0.5, 0.09375, ((0, 4),)),
        "high_up": bell_draw(own_keys[5], (RANK, D_INNER), RANK ** -0.5, 0.75, ((1, 2),)),
        "norm_train": jnp.clip(1.0 + 0.15 * jax.random.normal(own_keys[6], (D_MODEL,), jnp.float32), 0.25, 1.75),
        "norm_step": jnp.clip(jax.random.uniform(own_keys[7], (D_MODEL,), jnp.float32, -0.3, 0.3) * levels(own_keys[7], (D_MODEL,), ((0, 8),), -0.4, 0.0), -0.3, 0.3),
    }


mix_rate = 0.5


def reference(w_gate, low_gate, high_gate, w_up, low_up, high_up, norm_train, norm_step):
    fresh_gate = w_gate.astype(jnp.float32) + mix_rate * jnp.dot(low_gate, high_gate, preferred_element_type=jnp.float32)
    fresh_up = w_up.astype(jnp.float32) + mix_rate * jnp.dot(low_up, high_up, preferred_element_type=jnp.float32)
    column_gate = jnp.max(jnp.abs(fresh_gate), axis=0)
    serve_gate = (fresh_gate / column_gate).astype(jnp.bfloat16)
    column_up = jnp.max(jnp.abs(fresh_up), axis=0)
    serve_up = (fresh_up / column_up).astype(jnp.bfloat16)
    serve_norm = (norm_train + norm_step).astype(jnp.bfloat16)
    return serve_gate, serve_up, column_gate, column_up, serve_norm
```

```python
import functools

import jax
import jax.numpy as jnp
from jax import lax
from jax.experimental import pallas as pl
from jax.experimental.pallas import tpu as pltpu
from jax.sharding import PartitionSpec as P

mix_rate = 0.5
CHUNK = 256


def local_plain(w_gate, low_gate, high_gate, w_up, low_up, high_up, norm_train, norm_step):
    fresh_gate = w_gate.astype(jnp.float32) + mix_rate * jnp.dot(
        low_gate, high_gate, preferred_element_type=jnp.float32
    )
    fresh_up = w_up.astype(jnp.float32) + mix_rate * jnp.dot(
        low_up, high_up, preferred_element_type=jnp.float32
    )
    column_gate, column_up = lax.pmax(
        (jnp.max(jnp.abs(fresh_gate), axis=0), jnp.max(jnp.abs(fresh_up), axis=0)), "shard"
    )
    narrow_gate, narrow_up = (
        (fresh_gate / column_gate).astype(jnp.bfloat16),
        (fresh_up / column_up).astype(jnp.bfloat16),
    )
    serve_gate, serve_up = (
        lax.all_to_all(narrow_gate, "shard", split_axis=1, concat_axis=0, tiled=True),
        lax.all_to_all(narrow_up, "shard", split_axis=1, concat_axis=0, tiled=True),
    )
    place = lax.axis_index("shard")
    column_gate = lax.dynamic_slice_in_dim(
        column_gate, place * serve_gate.shape[1], serve_gate.shape[1]
    )
    column_up = lax.dynamic_slice_in_dim(column_up, place * serve_up.shape[1], serve_up.shape[1])
    serve_norm = lax.all_gather(
        (norm_train + norm_step).astype(jnp.bfloat16), ("shard", "width"), axis=0, tiled=True
    )
    return (serve_gate, serve_up, column_gate, column_up, serve_norm)


def exchange(
    n, nw, chunks, w_gate, w_up, low, high_gate, high_up, norm,
    out_gate, out_up, col_gate, col_up, norm_all,
    low_all, mix_gate, mix_up, fresh,
    send, recv, low_send, low_recv, fwd_send, fwd_recv, norm_send, norm_recv, own,
):
    me = lax.axis_index("shard")
    side = lax.axis_index("width")
    rows = w_gate.shape[0]
    cols = out_gate.shape[1]
    rank = high_gate.shape[0]
    half = rows // nw
    ws = (w_gate, w_up)
    outs = (out_gate, out_up)
    cuts = [(at, min(CHUNK, cols - at)) for at in range(0, cols, CHUNK)]
    others = [(a, b) for a in range(n) for b in range(nw) if (a, b) != (0, 0)]

    def peer(a, b):
        return {"shard": lax.rem(me + a, n), "width": lax.rem(side + b, nw)}

    barrier = pltpu.get_barrier_semaphore()
    for a, b in others:
        pl.semaphore_signal(
            barrier, inc=1, device_id=peer(a, b), device_id_type=pl.DeviceIdType.MESH
        )
    pl.semaphore_wait(barrier, len(others))

    def low_part(s, h):
        return pl.ds(pl.multiple_of(s * rows + h * half, 16), half)

    def low_copy(dst, s):
        return pltpu.make_async_remote_copy(
            src_ref=low.at[pl.ds(pl.multiple_of(side * half, 16), half)],
            dst_ref=low_all.at[low_part(s, side)],
            send_sem=low_send.at[dst], recv_sem=low_recv.at[s],
            device_id={"shard": dst, "width": side}, device_id_type=pl.DeviceIdType.MESH,
        )

    def low_forward(s, h, b):
        return pltpu.make_async_remote_copy(
            src_ref=low_all.at[low_part(s, h)], dst_ref=low_all.at[low_part(s, h)],
            send_sem=fwd_send.at[s, b], recv_sem=fwd_recv.at[s, b],
            device_id={"shard": me, "width": lax.rem(side + b, nw)},
            device_id_type=pl.DeviceIdType.MESH,
        )

    def piece(k, c, dst, s):
        at, wide = cuts[c]
        return pltpu.make_async_remote_copy(
            src_ref=ws[k].at[:, pl.ds(pl.multiple_of(dst * cols + at, 128), wide)],
            dst_ref=outs[k].at[pl.ds(pl.multiple_of(s * rows, 16), rows), pl.ds(at, wide)],
            send_sem=send.at[dst, k, c], recv_sem=recv.at[s, k, c],
            device_id={"shard": dst, "width": side}, device_id_type=pl.DeviceIdType.MESH,
        )

    def norm_copy(i, a, b, slot):
        return pltpu.make_async_remote_copy(
            src_ref=norm, dst_ref=norm_all.at[slot],
            send_sem=norm_send.at[i], recv_sem=norm_recv.at[i],
            device_id=peer(a, b), device_id_type=pl.DeviceIdType.MESH,
        )

    for d in range(1, n):
        for sign in (1, -1):
            dst = me + sign * d

            @pl.when((dst >= 0) & (dst < n))
            def _(dst=dst):
                low_copy(dst, me).start()

    slot = me * nw + side
    for i, (a, b) in enumerate(others):
        norm_copy(i, a, b, slot).start()

    for d in range(1, n):
        for k in range(2):
            for c in range(chunks):
                for sign in (1, -1):
                    dst = me + sign * d

                    @pl.when((dst >= 0) & (dst < n))
                    def _(dst=dst, k=k, c=c):
                        piece(k, c, dst, me).start()

    mine = pl.ds(pl.multiple_of(me * rows, 16), rows)
    my_cols = pl.ds(pl.multiple_of(me * cols, 128), cols)
    local = [
        pltpu.make_async_copy(w_gate.at[:, my_cols], out_gate.at[mine], own.at[0]),
        pltpu.make_async_copy(w_up.at[:, my_cols], out_up.at[mine], own.at[1]),
        pltpu.make_async_copy(low, low_all.at[mine], own.at[2]),
        pltpu.make_async_copy(high_gate.at[:, my_cols], mix_gate.at[pl.ds(0, rank)], own.at[3]),
        pltpu.make_async_copy(high_up.at[:, my_cols], mix_up.at[pl.ds(rank, rank)], own.at[4]),
        pltpu.make_async_copy(norm, norm_all.at[slot], own.at[5]),
    ]
    for copy in local:
        copy.start()
    mix_gate[rank:, :] = jnp.zeros((rank, cols), mix_gate.dtype)
    mix_up[:rank, :] = jnp.zeros((rank, cols), mix_up.dtype)

    for d in range(1, n):
        for sign in (1, -1):
            src = me + sign * d

            @pl.when((src >= 0) & (src < n))
            def _(src=src):
                low_copy(src, src).wait_recv()
                for b in range(1, nw):
                    low_forward(src, side, b).start()

    for copy in local:
        copy.wait()
    for d in range(1, n):
        for sign in (1, -1):
            src = me + sign * d

            @pl.when((src >= 0) & (src < n))
            def _(src=src):
                for b in range(1, nw):
                    low_forward(src, lax.rem(side + nw - b, nw), b).wait_recv()

    step = rows // 2
    for k, (out, mix, col) in enumerate(((out_gate, mix_gate, col_gate), (out_up, mix_up, col_up))):
        for c, (at, wide) in enumerate(cuts):
            for s in range(n):

                @pl.when(s != me)
                def _(s=s):
                    piece(k, c, s, s).wait_recv()

            here = pl.ds(at, wide)
            span = pl.ds(0, wide)

            def build(i, top):
                r = pl.ds(pl.multiple_of(i * step, 16), step)
                new = out[r, here].astype(jnp.float32) + mix_rate * jnp.dot(
                    low_all[r, :], mix[:, here], preferred_element_type=jnp.float32
                )
                fresh[r, span] = new
                return jnp.maximum(top, jnp.max(jnp.abs(new), axis=0, keepdims=True))

            top = lax.fori_loop(0, n * rows // step, build, jnp.zeros((1, wide), jnp.float32))
            col[:, here] = top
            inverse = 1.0 / top

            def scale(i, _):
                r = pl.ds(pl.multiple_of(i * step, 16), step)
                out[r, here] = (fresh[r, span] * inverse).astype(out.dtype)
                return 0

            lax.fori_loop(0, n * rows // step, scale, 0)

    for d in range(1, n):
        for sign in (1, -1):
            dst = me + sign * d

            @pl.when((dst >= 0) & (dst < n))
            def _(dst=dst):
                low_copy(dst, me).wait_send()
                for k in range(2):
                    for c in range(chunks):
                        piece(k, c, dst, me).wait_send()
                for b in range(1, nw):
                    low_forward(dst, side, b).wait_send()
    for i, (a, b) in enumerate(others):
        norm_copy(i, a, b, slot).wait()


def write_out(parts, gate, up, out_gate, out_up, sems):
    rows = gate.shape[0] // parts
    copies = [
        pltpu.make_async_copy(x.at[pl.ds(i * rows, rows)], y.at[pl.ds(i * rows, rows)], sems.at[k, i])
        for k, (x, y) in enumerate(((gate, out_gate), (up, out_up)))
        for i in range(parts)
    ]
    for copy in copies:
        copy.start()
    for copy in copies:
        copy.wait()


def local_kernel(n, nw, w_gate, low_gate, high_gate, w_up, low_up, high_up, norm_train, norm_step):
    rows = w_gate.shape[0]
    cols = w_gate.shape[1] // n
    rank = low_gate.shape[1]
    chunks = pl.cdiv(cols, CHUNK)
    size = norm_train.shape[0]
    low = jnp.concatenate([low_gate, low_up], axis=1)
    padded = pl.cdiv(size, 128) * 128
    norm = jnp.broadcast_to(jnp.pad(norm_train + norm_step, (0, padded - size))[None], (8, padded))
    hbm = pl.BlockSpec(memory_space=pl.ANY)
    vmem = pl.BlockSpec(memory_space=pltpu.VMEM)
    dma = pltpu.SemaphoreType.DMA
    gate, up, col_gate, col_up, norm_all = pl.pallas_call(
        functools.partial(exchange, n, nw, chunks),
        out_shape=(
            pltpu.VMEM((n * rows, cols), jnp.bfloat16),
            pltpu.VMEM((n * rows, cols), jnp.bfloat16),
            jax.ShapeDtypeStruct((1, cols), jnp.float32),
            jax.ShapeDtypeStruct((1, cols), jnp.float32),
            jax.ShapeDtypeStruct((n * nw, 8, padded), jnp.float32),
        ),
        in_specs=[hbm] * 6,
        out_specs=(vmem, vmem, vmem, vmem, hbm),
        scratch_shapes=[
            pltpu.VMEM((n * rows, 2 * rank), jnp.bfloat16),
            pltpu.VMEM((2 * rank, cols), jnp.bfloat16),
            pltpu.VMEM((2 * rank, cols), jnp.bfloat16),
            pltpu.VMEM((n * rows, CHUNK), jnp.float32),
            dma((n, 2, chunks)), dma((n, 2, chunks)),
            dma((n,)), dma((n,)),
            dma((n, nw)), dma((n, nw)),
            dma((n * nw,)), dma((n * nw,)),
            dma((6,)),
        ],
        compiler_params=pltpu.CompilerParams(
            collective_id=0, has_side_effects=True, vmem_limit_bytes=24 * 1024 * 1024
        ),
    )(w_gate, w_up, low, high_gate, high_up, norm)
    parts = 4
    serve_gate, serve_up = pl.pallas_call(
        functools.partial(write_out, parts),
        out_shape=(
            jax.ShapeDtypeStruct((n * rows, cols), jnp.bfloat16),
            jax.ShapeDtypeStruct((n * rows, cols), jnp.bfloat16),
        ),
        in_specs=[hbm, hbm],
        out_specs=(hbm, hbm),
        scratch_shapes=[dma((2, parts))],
        compiler_params=pltpu.CompilerParams(vmem_limit_bytes=8 * 1024 * 1024),
    )(gate, up)
    serve_norm = norm_all[:, 0, :size].reshape(-1).astype(jnp.bfloat16)
    return serve_gate, serve_up, col_gate[0], col_up[0], serve_norm


def solution(mesh):
    in_specs = (
        P(("unit", "shard"), "width"),
        P(("unit", "shard"), None),
        P("unit", "width"),
        P(("unit", "shard"), "width"),
        P(("unit", "shard"), None),
        P("unit", "width"),
        P(("unit", "shard", "width")),
        P(("unit", "shard", "width")),
    )
    out_specs = (
        P("unit", ("width", "shard")),
        P("unit", ("width", "shard")),
        P(("unit", "width", "shard")),
        P(("unit", "width", "shard")),
        P("unit"),
    )
    n, nw = mesh.shape["shard"], mesh.shape["width"]

    def local(*args):
        rows, cols = args[0].shape[0], args[0].shape[1] // n
        fits = (
            args[0].shape[1] % n == 0
            and cols % 128 == 0
            and rows % (16 * nw) == 0
            and n * rows * cols * 4 <= 32 * 2**20
            and 2 * args[1].shape[1] % 128 == 0
        )
        return local_kernel(n, nw, *args) if fits else local_plain(*args)

    return jax.shard_map(local, mesh=mesh, in_specs=in_specs, out_specs=out_specs, check_vma=False)
```
